32 devices in a mesh: groups: 2 (over y), grid: 4 (over z), depth: 4 (over x, core).
Axes of the slice: x: 2, y: 2, z: 4, core: 2. Of those that a mesh axis runs over, the one named last changes fastest.
Arguments:
- tokens: bfloat16 [512, 4096], P(('groups', 'grid'), 'depth'), parts along dimension 0, may hold values from -6 to 6
- gate_weight: bfloat16 [4096, 14336], P('depth', 'grid'), may hold values from -0.09375 to 0.09375
- up_weight: bfloat16 [4096, 14336], P('depth', 'grid'), may hold values from -0.09375 to 0.09375
- down_weight: bfloat16 [14336, 4096], P('grid', 'depth'), may hold values from -0.046875 to 0.046875
Outputs:
- mixed: bfloat16 [512, 4096], P(('groups', 'grid'), 'depth'), parts along dimension 0
The draws below stay inside these ranges and needn't reach their ends.
There are 2 independent parts, one for each index of `groups`. The reference program is written for one: setup_inputs(seed, part) draws one part's arguments, and reference() takes and returns one part's arrays. A program takes and returns all parts, laid end to end along the dimension named above; an argument that names none is the same for every part. Nothing has to cross between parts.
All inputs are finite; a program needn't handle non-finite values.
Results may differ from the reference program's by a relative error of at most 0.0049.
Values may be sent and summed in bfloat16 or wider, within the bound.
A program may use at most 64 MiB of HBM per device.

```python
import jax
import jax.numpy as jnp

D = 4096
FF = 14336
TOK = 256


def steps_of(rng, extent, pieces, low, largest):
    loudness, own = 1.0, jax.random.fold_in(rng, 6)
    for axis_at, shards_of in pieces:
        draws = jnp.exp(jax.random.uniform(jax.random.fold_in(own, axis_at), (shards_of,), jnp.float32, low / len(pieces), largest / len(pieces)))
        loudness = loudness * jnp.repeat(draws, extent[axis_at] // shards_of).reshape([-1 if axis == axis_at else 1 for axis in range(len(extent))])
    return loudness


def noise(stream_key, dims, spread, limit, split=(), kind=jnp.bfloat16):
    entries = jax.random.normal(stream_key, dims, jnp.float32) * spread
    if len(split) > 0:
        entries = steps_of(stream_key, dims, split, -0.22, 0.18) * entries
    return jnp.clip(entries, min=-limit, max=limit).astype(kind)


def setup_inputs(seed: int = 0, part: int = 0) -> dict:
    keys = jax.random.split(jax.random.key(seed), 5)
    own_keys = jax.random.split(jax.random.fold_in(keys[4], part), 5)
    return {
        "tokens": noise(own_keys[0], (TOK, D), 1.0, 6.0, ((0, 4), (1, 4))),
        "gate_weight": noise(keys[1], (D, FF), D ** -0.5, 0.09375, ((0, 4), (1, 4))),
        "up_weight": noise(keys[2], (D, FF), D ** -0.5, 0.09375, ((0, 4), (1, 4))),
        "down_weight": noise(keys[3], (FF, D), FF ** -0.5, 0.046875, ((0, 4), (1, 4))),
    }


def reference(tokens, gate_weight, up_weight, down_weight):
    gate = jnp.dot(tokens, gate_weight, preferred_element_type=jnp.float32)
    up = jnp.dot(tokens, up_weight, preferred_element_type=jnp.float32)
    hidden = (jax.nn.silu(gate) * up).astype(jnp.bfloat16)
    return jnp.dot(hidden, down_weight, preferred_element_type=jnp.float32).astype(jnp.bfloat16)
```

```python
import functools

import jax
import jax.numpy as jnp
from jax import lax
from jax.experimental import pallas as pl
from jax.experimental.pallas import tpu as pltpu
from jax.sharding import PartitionSpec as P

MESH = pl.DeviceIdType.MESH
FILL = (0, 3, 6, 9, 11)
STEADY = (0, 3, 6, 9, 11)
HEAD, NEXT, GAP = 5, 2, 0
DOWN_AT = 6


def flip(index, mask):
    out, bit = index, 1
    while bit <= mask:
        if mask & bit:
            out = out + bit - 2 * bit * lax.rem(lax.div(index, bit), 2)
        bit *= 2
    return out


def kernel(n, chunks, width, tokens, gate_w, up_w, down_w, out, tok, gate_v, up_v, down_v, part, core_out, core_in,
           chip_out, chip_in, hid, acc, grid_out, grid_in,
           w_sem, d_sem, tok_sem, toks_sem, tokr_sem, cores_sem, corer_sem, chips_sem, chipr_sem,
           hids_sem, hidr_sem, fwds_sem, fwdr_sem, grids_sem, gridr_sem):
    z, depth = lax.axis_index("grid"), lax.axis_index("depth")
    a, b = lax.div(depth, 2), lax.rem(depth, 2)
    other_core, other_chip = {"depth": depth + 1 - 2 * b}, {"depth": depth + 2 - 4 * a}
    peers = [{"grid": flip(z, mask)} for mask in [0, 1] + list(range(n - 1, 1, -1))]
    rows = tok.shape[1]
    half, quarter = rows // 2, rows // 4

    def span(core, chip):
        return pl.ds(pl.multiple_of(core * half + chip * quarter, quarter), quarter)

    my_rows, chip_rows = span(b, a), span(b, 1 - a)
    their_half = pl.ds(pl.multiple_of((1 - b) * half, half), half)
    sent = [my_rows, chip_rows, span(1 - b, a), span(1 - b, 1 - a)]
    units = n * chunks
    head = min(HEAD, chunks)
    ahead = chunks - head
    near = min(NEXT, chunks)
    filled = head + near
    back, last = filled + (n - 2) * chunks, head + (n - 1) * chunks
    entry = [0, head] + [filled + (c - 2) * chunks for c in range(2, n)]
    leave = [0, last - 1 if near < chunks else filled - 1] + [filled + (c - 1) * chunks - 1 for c in range(2, n)]

    def columns(k):
        return pl.ds(k * width if isinstance(k, int) else pl.multiple_of(k * width, width), width)

    def place(i):
        far = 2 + lax.div(jnp.maximum(i - filled, 0), chunks)
        s = jnp.where(i < head, 0, jnp.where(i < filled, 1, jnp.where(i < back, far, jnp.where(i < last, 1, 0))))
        return s, lax.rem(i + ahead, chunks)

    own = pltpu.make_async_copy(tokens, tok.at[0], tok_sem)
    own.start()

    def load(k):
        pltpu.make_async_copy(gate_w.at[:, columns(k)], gate_v.at[k], w_sem.at[2 * k]).start()
        pltpu.make_async_copy(up_w.at[:, columns(k)], up_v.at[k], w_sem.at[2 * k + 1]).start()

    for j in range(min(2, chunks)):
        load((ahead + j) % chunks)

    barrier = pltpu.get_barrier_semaphore()
    for peer in [other_core, other_chip] + peers[1:]:
        pl.semaphore_signal(barrier, inc=1, device_id=peer, device_id_type=MESH)
    acc[...] = jnp.zeros_like(acc)

    def tok_copy(s):
        return pltpu.make_async_remote_copy(
            tok.at[0], tok.at[s], toks_sem.at[s], tokr_sem.at[s], device_id=peers[s], device_id_type=MESH)

    def core_copy(i):
        return pltpu.make_async_remote_copy(
            core_out.at[i], core_in.at[i], cores_sem, corer_sem.at[i], device_id=other_core, device_id_type=MESH)

    def chip_copy(i):
        return pltpu.make_async_remote_copy(
            chip_out.at[i], chip_in.at[i], chips_sem, chipr_sem.at[i], device_id=other_chip, device_id_type=MESH)

    def hid_copy(i, at):
        return pltpu.make_async_remote_copy(
            hid.at[i, at], hid.at[i, at], hids_sem, hidr_sem.at[i], device_id=other_chip, device_id_type=MESH)

    def fwd_copy(i, at):
        return pltpu.make_async_remote_copy(
            hid.at[i, at], hid.at[i, at], fwds_sem, fwdr_sem.at[i], device_id=other_core, device_id_type=MESH)

    def grid_copy(s):
        return pltpu.make_async_remote_copy(
            grid_out.at[s], grid_in.at[s], grids_sem.at[s], gridr_sem.at[s], device_id=peers[s], device_id_type=MESH)

    def started():
        pl.semaphore_wait(barrier, n + 1)
        own.wait()
        for s in range(1, max(n - 1, 2)):
            tok_copy(s).start()

    def ready(t):
        s, k = place(t)
        for c in range(1, n):
            @pl.when(t == entry[c])
            def _():
                tok_copy(c).wait_recv()
                if c == 1 and n > 2:
                    tok_copy(n - 1).start()

        @pl.when(t < chunks)
        def _():
            pltpu.make_async_copy(gate_w.at[:, pl.ds(0, width)], gate_v.at[k], w_sem.at[2 * k]).wait()
            pltpu.make_async_copy(up_w.at[:, pl.ds(0, width)], up_v.at[k], w_sem.at[2 * k + 1]).wait()

    def project(t):
        s, k = place(t)
        x = jnp.concatenate([tok[s, at, :] for at in sent], axis=0)
        gate = jnp.dot(x, gate_v[k], preferred_element_type=jnp.float32)
        part[t, :, :width] = gate[:half]
        core_out[t, :, :width] = gate[half:]
        up = jnp.dot(x, up_v[k], preferred_element_type=jnp.float32)
        part[t, :, width:] = up[:half]
        core_out[t, :, width:] = up[half:]

    def reduce_core(i):
        chip_out[i] = (part[i, quarter:] + core_in[i, quarter:]).astype(jnp.bfloat16)

    def activate(i):
        summed = part[i, :quarter] + core_in[i, :quarter] + chip_in[i].astype(jnp.float32)
        g, u = summed[:, :width], summed[:, width:]
        hid[i, my_rows, :] = (g / (1.0 + jnp.exp(-g)) * u).astype(jnp.bfloat16)

    def down(i):
        s, k = place(i)
        acc[s] += jnp.dot(hid[i], down_v[k], preferred_element_type=jnp.float32)

    def step(offsets, loads, t, carry):
        dot, red, act, fwd, dwn = [None if o is None else t + o for o in offsets]
        if dot is not None:
            @pl.when(dot + 2 < chunks)
            def _():
                load(lax.rem(dot + ahead + 2, chunks))
        if loads:
            @pl.when(jnp.logical_and(t >= DOWN_AT, t < chunks + DOWN_AT))
            def _():
                k = lax.rem(t - DOWN_AT + ahead, chunks)
                pltpu.make_async_copy(down_w.at[columns(k), :], down_v.at[k], d_sem.at[k]).start()
        if red is not None:
            core_copy(red).wait_recv()
            reduce_core(red)
            chip_copy(red).start()
        if act is not None:
            chip_copy(act).wait_recv()
            activate(act)
            hid_copy(act, my_rows).start()
            fwd_copy(act, my_rows).start()
        if fwd is not None:
            hid_copy(fwd, chip_rows).wait_recv()
            fwd_copy(fwd, chip_rows).start()
        if dwn is not None:
            k = place(dwn)[1]

            @pl.when(dwn < chunks)
            def _():
                pltpu.make_async_copy(down_w.at[pl.ds(0, width), :], down_v.at[k], d_sem.at[k]).wait()

            fwd_copy(dwn, their_half).wait_recv()
        if dot is not None:
            ready(dot)
            project(dot)
        if dwn is not None:
            down(dwn)
        if dot is not None:
            core_copy(dot).start()
        if dwn is not None:
            for c in range(1, n):
                @pl.when(dwn == leave[c])
                def _():
                    grid_out[c] = acc[c].astype(jnp.bfloat16)
                    grid_copy(c).start()
        return carry

    started()
    plan = {}
    for i in range(units):
        for stage, lag in enumerate(FILL if i < filled else STEADY):
            t = i + lag + (0 if i < filled else GAP)
            plan.setdefault(t, [None] * 5)[stage] = i - t
    steps = [tuple(plan.get(t, [None] * 5)) for t in range(max(plan) + 1)]
    low = 0
    for t in range(1, len(steps) + 1):
        if t == len(steps) or steps[t] != steps[low]:
            loads = low < chunks + DOWN_AT and t > DOWN_AT
            lax.fori_loop(low, t, functools.partial(step, steps[low], loads), 0)
            low = t

    total = acc[0]
    for s in range(1, n):
        grid_copy(s).wait_recv()
        total = total + grid_in[s].astype(jnp.float32)
    out[...] = total.astype(out.dtype)

    for s in range(1, n):
        tok_copy(s).wait_send()
        grid_copy(s).wait_send()

    def drain(ref, sem, device):
        pltpu.make_async_remote_copy(
            ref, ref, sem, corer_sem.at[0], device_id=device, device_id_type=MESH).wait_send()

    drain(core_out, cores_sem, other_core)
    drain(chip_out, chips_sem, other_chip)
    drain(hid.at[:, my_rows], hids_sem, other_chip)
    drain(hid.at[:, their_half], fwds_sem, other_core)


def fused(n, width, tokens, gate_weight, up_weight, down_weight):
    rows, feats = tokens.shape
    share, outs = down_weight.shape
    chunks = share // width
    units = n * chunks
    vmem, dma = pltpu.VMEM, pltpu.SemaphoreType.DMA
    bf, f4 = jnp.bfloat16, jnp.float32
    return pl.pallas_call(
        functools.partial(kernel, n, chunks, width),
        out_shape=pltpu.VMEM((rows, outs), bf),
        in_specs=[pl.BlockSpec(memory_space=pl.ANY)] * 4,
        out_specs=pl.BlockSpec(memory_space=pltpu.VMEM),
        scratch_shapes=[
            vmem((n, rows, feats), bf),
            vmem((chunks, feats, width), bf),
            vmem((chunks, feats, width), bf),
            vmem((chunks, width, outs), bf),
            vmem((units, rows // 2, 2 * width), f4),
            vmem((units, rows // 2, 2 * width), f4),
            vmem((units, rows // 2, 2 * width), f4),
            vmem((units, rows // 4, 2 * width), bf),
            vmem((units, rows // 4, 2 * width), bf),
            vmem((units, rows, width), bf),
            vmem((n, rows, outs), f4),
            vmem((n, rows, outs), bf),
            vmem((n, rows, outs), bf),
            dma((2 * chunks,)), dma((chunks,)), dma, dma((n,)), dma((n,)),
            dma, dma((units,)), dma, dma((units,)),
            dma, dma((units,)), dma, dma((units,)), dma((n,)), dma((n,)),
        ],
        compiler_params=pltpu.CompilerParams(
            collective_id=0, has_side_effects=True, vmem_limit_bytes=60 * 1024 * 1024),
    )(tokens, gate_weight, up_weight, down_weight)


def plain(tokens, gate_weight, up_weight, down_weight):
    grid_size = lax.axis_size("grid")
    block_rows = tokens.shape[0]
    total_rows = block_rows * grid_size
    width_share = gate_weight.shape[1]
    stacked = jnp.concatenate([gate_weight, up_weight], axis=1)
    pre_act = jnp.dot(
        lax.all_gather(tokens, "grid", axis=0, tiled=True), stacked, preferred_element_type=jnp.float32)
    blocked = pre_act.reshape(grid_size, block_rows, 2 * width_share)
    summed = lax.psum_scatter(blocked, "depth", scatter_dimension=1, tiled=True)
    hidden = lax.all_gather(
        (jax.nn.silu(summed[..., :width_share]) * summed[..., width_share:]).astype(jnp.bfloat16),
        "depth", axis=1, tiled=True,
    ).reshape(total_rows, width_share)
    return lax.psum_scatter(
        jnp.dot(hidden, down_weight, preferred_element_type=jnp.float32),
        "grid", scatter_dimension=0, tiled=True,
    ).astype(jnp.bfloat16)


def body(tokens, gate_weight, up_weight, down_weight):
    n, depth = lax.axis_size("grid"), lax.axis_size("depth")
    rows, share = tokens.shape[0], gate_weight.shape[1]
    width = next((w for w in (512, 256) if share % w == 0), None)
    weights = 2 * (2 * gate_weight.size + down_weight.size)
    if depth == 4 and n in (2, 4, 8) and rows == 64 and width and weights < 32 * 2**20:
        return fused(n, width, tokens, gate_weight, up_weight, down_weight)
    return plain(tokens, gate_weight, up_weight, down_weight)


def solution(mesh):
    placed = (
        P(("groups", "grid"), "depth"),
        P("depth", "grid"),
        P("depth", "grid"),
        P("grid", "depth"),
    )
    return jax.shard_map(
        body, mesh=mesh, in_specs=placed, out_specs=P(("groups", "grid"), "depth"), check_vma=False
    )
```

```python
import functools

import jax
import jax.numpy as jnp
from jax import lax
from jax.experimental import pallas as pl
from jax.experimental.pallas import tpu as pltpu
from jax.sharding import PartitionSpec as P

MESH = pl.DeviceIdType.MESH
LAGS = (0, 3, 6, 9, 11)
HEAD = 5
NEAR = (4, 0)
LAUNCH = (5, 9)
DOWN_AT = 6


def flip(index, mask):
    out, bit = index, 1
    while bit <= mask:
        if mask & bit:
            out = out + bit - 2 * bit * lax.rem(lax.div(index, bit), 2)
        bit *= 2
    return out


def kernel(n, chunks, width, tokens, gate_w, up_w, down_w, out, tok, gate_v, up_v, down_v, part, core_out, core_in,
           chip_out, chip_in, hid, acc, grid_out, grid_in,
           w_sem, d_sem, tok_sem, toks_sem, tokr_sem, cores_sem, corer_sem, chips_sem, chipr_sem,
           hids_sem, hidr_sem, fwds_sem, fwdr_sem, grids_sem, gridr_sem):
    z, depth = lax.axis_index("grid"), lax.axis_index("depth")
    a, b = lax.div(depth, 2), lax.rem(depth, 2)
    other_core, other_chip = {"depth": depth + 1 - 2 * b}, {"depth": depth + 2 - 4 * a}
    peers = [{"grid": flip(z, mask)} for mask in [0, 1] + list(range(n - 1, 1, -1))]
    rows = tok.shape[1]
    half, quarter = rows // 2, rows // 4

    def span(core, chip):
        return pl.ds(pl.multiple_of(core * half + chip * quarter, quarter), quarter)

    my_rows, chip_rows = span(b, a), span(b, 1 - a)
    their_half = pl.ds(pl.multiple_of((1 - b) * half, half), half)
    sent = [my_rows, chip_rows, span(1 - b, a), span(1 - b, 1 - a)]
    units = n * chunks
    head = min(HEAD, chunks)
    ahead = chunks - head
    outer = jnp.logical_or(z == 0, z == n - 1)
    near = jnp.where(outer, *[min(count, chunks - 1) for count in NEAR])
    launch = jnp.where(outer, *LAUNCH)
    filled = head + near
    back, last = filled + (n - 2) * chunks, head + (n - 1) * chunks
    entry = [0, jnp.where(near > 0, head, back)] + [filled + (c - 2) * chunks for c in range(2, n)]
    leave = [0, last - 1] + [filled + (c - 1) * chunks - 1 for c in range(2, n)]

    def columns(k):
        return pl.ds(k * width if isinstance(k, int) else pl.multiple_of(k * width, width), width)

    def place(i):
        far = 2 + lax.div(jnp.maximum(i - filled, 0), chunks)
        s = jnp.where(i < head, 0, jnp.where(i < filled, 1, jnp.where(i < back, far, jnp.where(i < last, 1, 0))))
        return s, lax.rem(i + ahead, chunks)

    own = pltpu.make_async_copy(tokens, tok.at[0], tok_sem)
    own.start()

    def load(k):
        pltpu.make_async_copy(gate_w.at[:, columns(k)], gate_v.at[k], w_sem.at[2 * k]).start()
        pltpu.make_async_copy(up_w.at[:, columns(k)], up_v.at[k], w_sem.at[2 * k + 1]).start()

    for j in range(min(2, chunks)):
        load((ahead + j) % chunks)

    barrier = pltpu.get_barrier_semaphore()
    for peer in [other_core, other_chip] + peers[1:]:
        pl.semaphore_signal(barrier, inc=1, device_id=peer, device_id_type=MESH)
    acc[...] = jnp.zeros_like(acc)

    def tok_copy(s):
        return pltpu.make_async_remote_copy(
            tok.at[0], tok.at[s], toks_sem.at[s], tokr_sem.at[s], device_id=peers[s], device_id_type=MESH)

    def core_copy(i):
        return pltpu.make_async_remote_copy(
            core_out.at[i], core_in.at[i], cores_sem, corer_sem.at[i], device_id=other_core, device_id_type=MESH)

    def chip_copy(i):
        return pltpu.make_async_remote_copy(
            chip_out.at[i], chip_in.at[i], chips_sem, chipr_sem.at[i], device_id=other_chip, device_id_type=MESH)

    def hid_copy(i, at):
        return pltpu.make_async_remote_copy(
            hid.at[i, at], hid.at[i, at], hids_sem, hidr_sem.at[i], device_id=other_chip, device_id_type=MESH)

    def fwd_copy(i, at):
        return pltpu.make_async_remote_copy(
            hid.at[i, at], hid.at[i, at], fwds_sem, fwdr_sem.at[i], device_id=other_core, device_id_type=MESH)

    def grid_copy(s):
        return pltpu.make_async_remote_copy(
            grid_out.at[s], grid_in.at[s], grids_sem.at[s], gridr_sem.at[s], device_id=peers[s], device_id_type=MESH)

    def started():
        pl.semaphore_wait(barrier, n + 1)
        own.wait()
        for s in range(1, max(n - 1, 2)):
            tok_copy(s).start()

    def ready(t):
        s, k = place(t)
        if n > 2:
            @pl.when(t == launch)
            def _():
                tok_copy(n - 1).start()

        for c in range(1, n):
            @pl.when(t == entry[c])
            def _():
                tok_copy(c).wait_recv()

        @pl.when(t < chunks)
        def _():
            pltpu.make_async_copy(gate_w.at[:, pl.ds(0, width)], gate_v.at[k], w_sem.at[2 * k]).wait()
            pltpu.make_async_copy(up_w.at[:, pl.ds(0, width)], up_v.at[k], w_sem.at[2 * k + 1]).wait()

    def project(t):
        s, k = place(t)
        x = jnp.concatenate([tok[s, at, :] for at in sent], axis=0)
        gate = jnp.dot(x, gate_v[k], preferred_element_type=jnp.float32)
        part[t, :, :width] = gate[:half]
        core_out[t, :, :width] = gate[half:]
        up = jnp.dot(x, up_v[k], preferred_element_type=jnp.float32)
        part[t, :, width:] = up[:half]
        core_out[t, :, width:] = up[half:]

    def reduce_core(i):
        chip_out[i] = (part[i, quarter:] + core_in[i, quarter:]).astype(jnp.bfloat16)

    def activate(i):
        summed = part[i, :quarter] + core_in[i, :quarter] + chip_in[i].astype(jnp.float32)
        g, u = summed[:, :width], summed[:, width:]
        hid[i, my_rows, :] = (g / (1.0 + jnp.exp(-g)) * u).astype(jnp.bfloat16)

    def down(i):
        s, k = place(i)
        acc[s] += jnp.dot(hid[i], down_v[k], preferred_element_type=jnp.float32)

    def step(offsets, loads, t, carry):
        dot, red, act, fwd, dwn = [None if o is None else t + o for o in offsets]
        if dot is not None:
            @pl.when(dot + 2 < chunks)
            def _():
                load(lax.rem(dot + ahead + 2, chunks))
        if loads:
            @pl.when(jnp.logical_and(t >= DOWN_AT, t < chunks + DOWN_AT))
            def _():
                k = lax.rem(t - DOWN_AT + ahead, chunks)
                pltpu.make_async_copy(down_w.at[columns(k), :], down_v.at[k], d_sem.at[k]).start()
        if red is not None:
            core_copy(red).wait_recv()
            reduce_core(red)
            chip_copy(red).start()
        if act is not None:
            chip_copy(act).wait_recv()
            activate(act)
            hid_copy(act, my_rows).start()
            fwd_copy(act, my_rows).start()
        if fwd is not None:
            hid_copy(fwd, chip_rows).wait_recv()
            fwd_copy(fwd, chip_rows).start()
        if dwn is not None:
            k = place(dwn)[1]

            @pl.when(dwn < chunks)
            def _():
                pltpu.make_async_copy(down_w.at[pl.ds(0, width), :], down_v.at[k], d_sem.at[k]).wait()

            fwd_copy(dwn, their_half).wait_recv()
        if dot is not None:
            ready(dot)
            project(dot)
        if dwn is not None:
            down(dwn)
        if dot is not None:
            core_copy(dot).start()
        if dwn is not None:
            for c in range(1, n):
                @pl.when(dwn == leave[c])
                def _():
                    grid_out[c] = acc[c].astype(jnp.bfloat16)
                    grid_copy(c).start()
        return carry

    started()
    plan = {}
    for i in range(units):
        for stage, lag in enumerate(LAGS):
            plan.setdefault(i + lag, [None] * 5)[stage] = -lag
    steps = [tuple(plan.get(t, [None] * 5)) for t in range(max(plan) + 1)]
    low = 0
    for t in range(1, len(steps) + 1):
        if t == len(steps) or steps[t] != steps[low]:
            loads = low < chunks + DOWN_AT and t > DOWN_AT
            lax.fori_loop(low, t, functools.partial(step, steps[low], loads), 0)
            low = t

    total = acc[0]
    for s in range(1, n):
        grid_copy(s).wait_recv()
        total = total + grid_in[s].astype(jnp.float32)
    out[...] = total.astype(out.dtype)

    for s in range(1, n):
        tok_copy(s).wait_send()
        grid_copy(s).wait_send()

    def drain(ref, sem, device):
        pltpu.make_async_remote_copy(
            ref, ref, sem, corer_sem.at[0], device_id=device, device_id_type=MESH).wait_send()

    drain(core_out, cores_sem, other_core)
    drain(chip_out, chips_sem, other_chip)
    drain(hid.at[:, my_rows], hids_sem, other_chip)
    drain(hid.at[:, their_half], fwds_sem, other_core)


def fused(n, width, tokens, gate_weight, up_weight, down_weight):
    rows, feats = tokens.shape
    share, outs = down_weight.shape
    chunks = share // width
    units = n * chunks
    vmem, dma = pltpu.VMEM, pltpu.SemaphoreType.DMA
    bf, f4 = jnp.bfloat16, jnp.float32
    return pl.pallas_call(
        functools.partial(kernel, n, chunks, width),
        out_shape=pltpu.VMEM((rows, outs), bf),
        in_specs=[pl.BlockSpec(memory_space=pl.ANY)] * 4,
        out_specs=pl.BlockSpec(memory_space=pltpu.VMEM),
        scratch_shapes=[
            vmem((n, rows, feats), bf),
            vmem((chunks, feats, width), bf),
            vmem((chunks, feats, width), bf),
            vmem((chunks, width, outs), bf),
            vmem((units, rows // 2, 2 * width), f4),
            vmem((units, rows // 2, 2 * width), f4),
            vmem((units, rows // 2, 2 * width), f4),
            vmem((units, rows // 4, 2 * width), bf),
            vmem((units, rows // 4, 2 * width), bf),
            vmem((units, rows, width), bf),
            vmem((n, rows, outs), f4),
            vmem((n, rows, outs), bf),
            vmem((n, rows, outs), bf),
            dma((2 * chunks,)), dma((chunks,)), dma, dma((n,)), dma((n,)),
            dma, dma((units,)), dma, dma((units,)),
            dma, dma((units,)), dma, dma((units,)), dma((n,)), dma((n,)),
        ],
        compiler_params=pltpu.CompilerParams(
            collective_id=0, has_side_effects=True, vmem_limit_bytes=60 * 1024 * 1024),
    )(tokens, gate_weight, up_weight, down_weight)


def plain(tokens, gate_weight, up_weight, down_weight):
    grid_size = lax.axis_size("grid")
    block_rows = tokens.shape[0]
    total_rows = block_rows * grid_size
    width_share = gate_weight.shape[1]
    stacked = jnp.concatenate([gate_weight, up_weight], axis=1)
    pre_act = jnp.dot(
        lax.all_gather(tokens, "grid", axis=0, tiled=True), stacked, preferred_element_type=jnp.float32)
    blocked = pre_act.reshape(grid_size, block_rows, 2 * width_share)
    summed = lax.psum_scatter(blocked, "depth", scatter_dimension=1, tiled=True)
    hidden = lax.all_gather(
        (jax.nn.silu(summed[..., :width_share]) * summed[..., width_share:]).astype(jnp.bfloat16),
        "depth", axis=1, tiled=True,
    ).reshape(total_rows, width_share)
    return lax.psum_scatter(
        jnp.dot(hidden, down_weight, preferred_element_type=jnp.float32),
        "grid", scatter_dimension=0, tiled=True,
    ).astype(jnp.bfloat16)


def body(tokens, gate_weight, up_weight, down_weight):
    n, depth = lax.axis_size("grid"), lax.axis_size("depth")
    rows, share = tokens.shape[0], gate_weight.shape[1]
    width = next((w for w in (512, 256) if share % w == 0), None)
    weights = 2 * (2 * gate_weight.size + down_weight.size)
    if depth == 4 and n in (2, 4, 8) and rows == 64 and width and weights < 32 * 2**20:
        return fused(n, width, tokens, gate_weight, up_weight, down_weight)
    return plain(tokens, gate_weight, up_weight, down_weight)


def solution(mesh):
    placed = (
        P(("groups", "grid"), "depth"),
        P("depth", "grid"),
        P("depth", "grid"),
        P("grid", "depth"),
    )
    return jax.shard_map(
        body, mesh=mesh, in_specs=placed, out_specs=P(("groups", "grid"), "depth"), check_vma=False
    )
```

```python
import functools

import jax
import jax.numpy as jnp
from jax import lax
from jax.experimental import pallas as pl
from jax.experimental.pallas import tpu as pltpu
from jax.sharding import PartitionSpec as P

MESH = pl.DeviceIdType.MESH
LAGS = (0, 3, 6, 9, 11)
HEAD = 5
NEAR = (4, 0)
LAUNCH = (5, 9)
DOWN_AT = 6
RING = 12


def flip(index, mask):
    out, bit = index, 1
    while bit <= mask:
        if mask & bit:
            out = out + bit - 2 * bit * lax.rem(lax.div(index, bit), 2)
        bit *= 2
    return out


def kernel(n, chunks, width, tokens, gate_w, up_w, down_w, out, tok, gate_v, up_v, down_v, part, core_out, core_in,
           chip_out, chip_in, hid, acc, grid_out, grid_in,
           w_sem, d_sem, tok_sem, toks_sem, tokr_sem, cores_sem, corer_sem, chips_sem, chipr_sem,
           hids_sem, hidr_sem, fwds_sem, fwdr_sem, grids_sem, gridr_sem):
    z, depth = lax.axis_index("grid"), lax.axis_index("depth")
    a, b = lax.div(depth, 2), lax.rem(depth, 2)
    other_core, other_chip = {"depth": depth + 1 - 2 * b}, {"depth": depth + 2 - 4 * a}
    peers = [{"grid": flip(z, mask)} for mask in [0, 1] + list(range(n - 1, 1, -1))]
    rows = tok.shape[1]
    half, quarter = rows // 2, rows // 4

    def span(core, chip):
        return pl.ds(pl.multiple_of(core * half + chip * quarter, quarter), quarter)

    my_rows, chip_rows = span(b, a), span(b, 1 - a)
    their_half = pl.ds(pl.multiple_of((1 - b) * half, half), half)
    sent = [my_rows, chip_rows, span(1 - b, a), span(1 - b, 1 - a)]
    units = n * chunks
    head = min(HEAD, chunks)
    ahead = chunks - head
    outer = jnp.logical_or(z == 0, z == n - 1)
    near = jnp.where(outer, *[min(count, chunks - 1) for count in NEAR])
    launch = jnp.where(outer, *LAUNCH)
    filled = head + near
    back, last = filled + (n - 2) * chunks, head + (n - 1) * chunks
    entry = [0, jnp.where(near > 0, head, back)] + [filled + (c - 2) * chunks for c in range(2, n)]
    leave = [0, last - 1] + [filled + (c - 1) * chunks - 1 for c in range(2, n)]

    def columns(k):
        return pl.ds(k * width if isinstance(k, int) else pl.multiple_of(k * width, width), width)

    def place(i):
        far = 2 + lax.div(jnp.maximum(i - filled, 0), chunks)
        s = jnp.where(i < head, 0, jnp.where(i < filled, 1, jnp.where(i < back, far, jnp.where(i < last, 1, 0))))
        return s, lax.rem(i + ahead, chunks)

    own = pltpu.make_async_copy(tokens, tok.at[0], tok_sem)
    own.start()

    def load(k):
        pltpu.make_async_copy(gate_w.at[:, columns(k)], gate_v.at[k], w_sem.at[2 * k]).start()
        pltpu.make_async_copy(up_w.at[:, columns(k)], up_v.at[k], w_sem.at[2 * k + 1]).start()

    for j in range(min(2, chunks)):
        load((ahead + j) % chunks)

    barrier = pltpu.get_barrier_semaphore()
    for peer in [other_core, other_chip] + peers[1:]:
        pl.semaphore_signal(barrier, inc=1, device_id=peer, device_id_type=MESH)
    acc[...] = jnp.zeros_like(acc)

    def tok_copy(s):
        return pltpu.make_async_remote_copy(
            tok.at[0], tok.at[s], toks_sem.at[s], tokr_sem.at[s], device_id=peers[s], device_id_type=MESH)

    def core_copy(i):
        return pltpu.make_async_remote_copy(
            core_out.at[i], core_in.at[i], cores_sem, corer_sem.at[lax.rem(i, RING)], device_id=other_core, device_id_type=MESH)

    def chip_copy(i):
        return pltpu.make_async_remote_copy(
            chip_out.at[i], chip_in.at[i], chips_sem, chipr_sem.at[lax.rem(i, RING)], device_id=other_chip, device_id_type=MESH)

    def hid_copy(i, at):
        return pltpu.make_async_remote_copy(
            hid.at[i, at], hid.at[i, at], hids_sem, hidr_sem.at[lax.rem(i, RING)], device_id=other_chip, device_id_type=MESH)

    def fwd_copy(i, at):
        return pltpu.make_async_remote_copy(
            hid.at[i, at], hid.at[i, at], fwds_sem, fwdr_sem.at[lax.rem(i, RING)], device_id=other_core, device_id_type=MESH)

    def grid_copy(s):
        return pltpu.make_async_remote_copy(
            grid_out.at[s], grid_in.at[s], grids_sem.at[s], gridr_sem.at[s], device_id=peers[s], device_id_type=MESH)

    def started():
        pl.semaphore_wait(barrier, n + 1)
        own.wait()
        for s in range(1, max(n - 1, 2)):
            tok_copy(s).start()

    def ready(t):
        s, k = place(t)
        if n > 2:
            @pl.when(t == launch)
            def _():
                tok_copy(n - 1).start()

        for c in range(1, n):
            @pl.when(t == entry[c])
            def _():
                tok_copy(c).wait_recv()

        @pl.when(t < chunks)
        def _():
            pltpu.make_async_copy(gate_w.at[:, pl.ds(0, width)], gate_v.at[k], w_sem.at[2 * k]).wait()
            pltpu.make_async_copy(up_w.at[:, pl.ds(0, width)], up_v.at[k], w_sem.at[2 * k + 1]).wait()

    def project(t):
        s, k = place(t)
        x = jnp.concatenate([tok[s, at, :] for at in sent], axis=0)
        gate = jnp.dot(x, gate_v[k], preferred_element_type=jnp.float32)
        part[t, :, :width] = gate[:half]
        core_out[t, :, :width] = gate[half:]
        up = jnp.dot(x, up_v[k], preferred_element_type=jnp.float32)
        part[t, :, width:] = up[:half]
        core_out[t, :, width:] = up[half:]

    def reduce_core(i):
        chip_out[i] = (part[i, quarter:] + core_in[i, quarter:]).astype(jnp.bfloat16)

    def activate(i):
        summed = part[i, :quarter] + core_in[i, :quarter] + chip_in[i].astype(jnp.float32)
        g, u = summed[:, :width], summed[:, width:]
        hid[i, my_rows, :] = (g / (1.0 + jnp.exp(-g)) * u).astype(jnp.bfloat16)

    def down(i):
        s, k = place(i)
        acc[s] += jnp.dot(hid[i], down_v[k], preferred_element_type=jnp.float32)

    def step(offsets, loads, t, carry):
        dot, red, act, fwd, dwn = [None if o is None else t + o for o in offsets]
        if dot is not None:
            @pl.when(dot + 2 < chunks)
            def _():
                load(lax.rem(dot + ahead + 2, chunks))
        if loads:
            @pl.when(jnp.logical_and(t >= DOWN_AT, t < chunks + DOWN_AT))
            def _():
                k = lax.rem(t - DOWN_AT + ahead, chunks)
                pltpu.make_async_copy(down_w.at[columns(k), :], down_v.at[k], d_sem.at[k]).start()
        if red is not None:
            core_copy(red).wait_recv()
            reduce_core(red)
            chip_copy(red).start()
        if act is not None:
            chip_copy(act).wait_recv()
            activate(act)
            hid_copy(act, my_rows).start()
            fwd_copy(act, my_rows).start()
        if fwd is not None:
            hid_copy(fwd, chip_rows).wait_recv()
            fwd_copy(fwd, chip_rows).start()
        if dwn is not None:
            k = place(dwn)[1]

            @pl.when(dwn < chunks)
            def _():
                pltpu.make_async_copy(down_w.at[pl.ds(0, width), :], down_v.at[k], d_sem.at[k]).wait()

            fwd_copy(dwn, their_half).wait_recv()
        if dot is not None:
            ready(dot)
            project(dot)
        if dwn is not None:
            down(dwn)
        if dot is not None:
            core_copy(dot).start()
        if dwn is not None:
            for c in range(1, n):
                @pl.when(dwn == leave[c])
                def _():
                    grid_out[c] = acc[c].astype(jnp.bfloat16)
                    grid_copy(c).start()
        return carry

    started()
    plan = {}
    for i in range(units):
        for stage, lag in enumerate(LAGS):
            plan.setdefault(i + lag, [None] * 5)[stage] = -lag
    steps = [tuple(plan.get(t, [None] * 5)) for t in range(max(plan) + 1)]
    low = 0
    for t in range(1, len(steps) + 1):
        if t == len(steps) or steps[t] != steps[low]:
            loads = low < chunks + DOWN_AT and t > DOWN_AT
            lax.fori_loop(low, t, functools.partial(step, steps[low], loads), 0)
            low = t

    total = acc[0]
    for s in range(1, n):
        grid_copy(s).wait_recv()
        total = total + grid_in[s].astype(jnp.float32)
    out[...] = total.astype(out.dtype)

    for s in range(1, n):
        tok_copy(s).wait_send()
        grid_copy(s).wait_send()

    def drain(ref, sem, device):
        pltpu.make_async_remote_copy(
            ref, ref, sem, corer_sem.at[0], device_id=device, device_id_type=MESH).wait_send()

    drain(core_out, cores_sem, other_core)
    drain(chip_out, chips_sem, other_chip)
    drain(hid.at[:, my_rows], hids_sem, other_chip)
    drain(hid.at[:, their_half], fwds_sem, other_core)


def fused(n, width, tokens, gate_weight, up_weight, down_weight):
    rows, feats = tokens.shape
    share, outs = down_weight.shape
    chunks = share // width
    units = n * chunks
    vmem, dma = pltpu.VMEM, pltpu.SemaphoreType.DMA
    bf, f4 = jnp.bfloat16, jnp.float32
    return pl.pallas_call(
        functools.partial(kernel, n, chunks, width),
        out_shape=pltpu.VMEM((rows, outs), bf),
        in_specs=[pl.BlockSpec(memory_space=pl.ANY)] * 4,
        out_specs=pl.BlockSpec(memory_space=pltpu.VMEM),
        scratch_shapes=[
            vmem((n, rows, feats), bf),
            vmem((chunks, feats, width), bf),
            vmem((chunks, feats, width), bf),
            vmem((chunks, width, outs), bf),
            vmem((units, rows // 2, 2 * width), f4),
            vmem((units, rows // 2, 2 * width), f4),
            vmem((units, rows // 2, 2 * width), f4),
            vmem((units, rows // 4, 2 * width), bf),
            vmem((units, rows // 4, 2 * width), bf),
            vmem((units, rows, width), bf),
            vmem((n, rows, outs), f4),
            vmem((n, rows, outs), bf),
            vmem((n, rows, outs), bf),
            dma((2 * chunks,)), dma((chunks,)), dma, dma((n,)), dma((n,)),
            dma, dma((RING,)), dma, dma((RING,)),
            dma, dma((RING,)), dma, dma((RING,)), dma((n,)), dma((n,)),
        ],
        compiler_params=pltpu.CompilerParams(
            collective_id=0, has_side_effects=True, vmem_limit_bytes=60 * 1024 * 1024),
    )(tokens, gate_weight, up_weight, down_weight)


def plain(tokens, gate_weight, up_weight, down_weight):
    grid_size = lax.axis_size("grid")
    block_rows = tokens.shape[0]
    total_rows = block_rows * grid_size
    width_share = gate_weight.shape[1]
    stacked = jnp.concatenate([gate_weight, up_weight], axis=1)
    pre_act = jnp.dot(
        lax.all_gather(tokens, "grid", axis=0, tiled=True), stacked, preferred_element_type=jnp.float32)
    blocked = pre_act.reshape(grid_size, block_rows, 2 * width_share)
    summed = lax.psum_scatter(blocked, "depth", scatter_dimension=1, tiled=True)
    hidden = lax.all_gather(
        (jax.nn.silu(summed[..., :width_share]) * summed[..., width_share:]).astype(jnp.bfloat16),
        "depth", axis=1, tiled=True,
    ).reshape(total_rows, width_share)
    return lax.psum_scatter(
        jnp.dot(hidden, down_weight, preferred_element_type=jnp.float32),
        "grid", scatter_dimension=0, tiled=True,
    ).astype(jnp.bfloat16)


def body(tokens, gate_weight, up_weight, down_weight):
    n, depth = lax.axis_size("grid"), lax.axis_size("depth")
    rows, share = tokens.shape[0], gate_weight.shape[1]
    width = next((w for w in (512, 256) if share % w == 0), None)
    weights = 2 * (2 * gate_weight.size + down_weight.size)
    if depth == 4 and n in (2, 4, 8) and rows == 64 and width and weights < 32 * 2**20:
        return fused(n, width, tokens, gate_weight, up_weight, down_weight)
    return plain(tokens, gate_weight, up_weight, down_weight)


def solution(mesh):
    placed = (
        P(("groups", "grid"), "depth"),
        P("depth", "grid"),
        P("depth", "grid"),
        P("grid", "depth"),
    )
    return jax.shard_map(
        body, mesh=mesh, in_specs=placed, out_specs=P(("groups", "grid"), "depth"), check_vma=False
    )
```

```python
import functools

import jax
import jax.numpy as jnp
from jax import lax
from jax.experimental import pallas as pl
from jax.experimental.pallas import tpu as pltpu
from jax.sharding import PartitionSpec as P

MESH = pl.DeviceIdType.MESH
LAGS = (0, 3, 6, 9, 10)
HEAD = (4, 5)
NEAR = (5, 0)
LAUNCH = (5, 9)
DOWN_AT = 6
RING = 11
FIRST, DEEP = 2, 4


def flip(index, mask):
    out, bit = index, 1
    while bit <= mask:
        if mask & bit:
            out = out + bit - 2 * bit * lax.rem(lax.div(index, bit), 2)
        bit *= 2
    return out


def kernel(n, chunks, width, tokens, gate_w, up_w, down_w, out, tok, gate_v, up_v, down_v, part, core_out, core_in,
           chip_out, chip_in, hid, acc, grid_out, grid_in,
           w_sem, d_sem, tok_sem, toks_sem, tokr_sem, cores_sem, corer_sem, chips_sem, chipr_sem,
           hids_sem, hidr_sem, fwds_sem, fwdr_sem, grids_sem, gridr_sem):
    z, depth = lax.axis_index("grid"), lax.axis_index("depth")
    a, b = lax.div(depth, 2), lax.rem(depth, 2)
    other_core, other_chip = {"depth": depth + 1 - 2 * b}, {"depth": depth + 2 - 4 * a}
    peers = [{"grid": flip(z, mask)} for mask in [0, 1] + list(range(n - 1, 1, -1))]
    rows = tok.shape[1]
    half, quarter = rows // 2, rows // 4

    def span(core, chip):
        return pl.ds(pl.multiple_of(core * half + chip * quarter, quarter), quarter)

    my_rows, chip_rows = span(b, a), span(b, 1 - a)
    their_half = pl.ds(pl.multiple_of((1 - b) * half, half), half)
    sent = [my_rows, chip_rows, span(1 - b, a), span(1 - b, 1 - a)]
    units = n * chunks
    ahead = chunks - min(max(HEAD), chunks)
    outer = jnp.logical_or(z == 0, z == n - 1)
    head = jnp.where(outer, *[min(count, chunks) for count in HEAD])
    near = jnp.where(outer, *[min(count, chunks - 1) for count in NEAR])
    launch = jnp.where(outer, *LAUNCH)
    filled = head + near
    back, last = filled + (n - 2) * chunks, head + (n - 1) * chunks
    entry = [0, jnp.where(near > 0, head, back)] + [filled + (c - 2) * chunks for c in range(2, n)]
    leave = [0, last - 1] + [filled + (c - 1) * chunks - 1 for c in range(2, n)]

    def columns(k):
        return pl.ds(k * width if isinstance(k, int) else pl.multiple_of(k * width, width), width)

    def place(i):
        far = 2 + lax.div(jnp.maximum(i - filled, 0), chunks)
        s = jnp.where(i < head, 0, jnp.where(i < filled, 1, jnp.where(i < back, far, jnp.where(i < last, 1, 0))))
        return s, lax.rem(i + ahead, chunks)

    own = pltpu.make_async_copy(tokens, tok.at[0], tok_sem)
    own.start()

    def load(k):
        pltpu.make_async_copy(gate_w.at[:, columns(k)], gate_v.at[k], w_sem.at[2 * k]).start()
        pltpu.make_async_copy(up_w.at[:, columns(k)], up_v.at[k], w_sem.at[2 * k + 1]).start()

    for j in range(min(FIRST, chunks)):
        load((ahead + j) % chunks)

    barrier = pltpu.get_barrier_semaphore()
    for peer in [other_core, other_chip] + peers[1:]:
        pl.semaphore_signal(barrier, inc=1, device_id=peer, device_id_type=MESH)
    acc[...] = jnp.zeros_like(acc)

    def tok_copy(s):
        return pltpu.make_async_remote_copy(
            tok.at[0], tok.at[s], toks_sem.at[s], tokr_sem.at[s], device_id=peers[s], device_id_type=MESH)

    def core_copy(i):
        return pltpu.make_async_remote_copy(
            core_out.at[i], core_in.at[i], cores_sem, corer_sem.at[lax.rem(i, RING)], device_id=other_core, device_id_type=MESH)

    def chip_copy(i):
        return pltpu.make_async_remote_copy(
            chip_out.at[i], chip_in.at[i], chips_sem, chipr_sem.at[lax.rem(i, RING)], device_id=other_chip, device_id_type=MESH)

    def hid_copy(i, at):
        return pltpu.make_async_remote_copy(
            hid.at[i, at], hid.at[i, at], hids_sem, hidr_sem.at[lax.rem(i, RING)], device_id=other_chip, device_id_type=MESH)

    def fwd_copy(i, at):
        return pltpu.make_async_remote_copy(
            hid.at[i, at], hid.at[i, at], fwds_sem, fwdr_sem.at[lax.rem(i, RING)], device_id=other_core, device_id_type=MESH)

    def grid_copy(s):
        return pltpu.make_async_remote_copy(
            grid_out.at[s], grid_in.at[s], grids_sem.at[s], gridr_sem.at[s], device_id=peers[s], device_id_type=MESH)

    def started():
        pl.semaphore_wait(barrier, n + 1)
        own.wait()
        for s in range(1, max(n - 1, 2)):
            tok_copy(s).start()
        for j in range(min(FIRST, chunks), min(DEEP, chunks)):
            load((ahead + j) % chunks)

    def ready(t):
        s, k = place(t)
        if n > 2:
            @pl.when(t == launch)
            def _():
                tok_copy(n - 1).start()

        for c in range(1, n):
            @pl.when(t == entry[c])
            def _():
                tok_copy(c).wait_recv()

        @pl.when(t < chunks)
        def _():
            pltpu.make_async_copy(gate_w.at[:, pl.ds(0, width)], gate_v.at[k], w_sem.at[2 * k]).wait()
            pltpu.make_async_copy(up_w.at[:, pl.ds(0, width)], up_v.at[k], w_sem.at[2 * k + 1]).wait()

    def project(t):
        s, k = place(t)
        x = jnp.concatenate([tok[s, at, :] for at in sent], axis=0)
        gate = jnp.dot(x, gate_v[k], preferred_element_type=jnp.float32)
        part[t, :, :width] = gate[:half]
        core_out[t, :, :width] = gate[half:]
        up = jnp.dot(x, up_v[k], preferred_element_type=jnp.float32)
        part[t, :, width:] = up[:half]
        core_out[t, :, width:] = up[half:]

    def reduce_core(i):
        chip_out[i] = (part[i, quarter:] + core_in[i, quarter:]).astype(jnp.bfloat16)

    def activate(i):
        summed = part[i, :quarter] + core_in[i, :quarter] + chip_in[i].astype(jnp.float32)
        g, u = summed[:, :width], summed[:, width:]
        hid[i, my_rows, :] = (g / (1.0 + jnp.exp(-g)) * u).astype(jnp.bfloat16)

    def down(i):
        s, k = place(i)
        acc[s] += jnp.dot(hid[i], down_v[k], preferred_element_type=jnp.float32)

    def step(offsets, loads, t, carry):
        dot, red, act, fwd, dwn = [None if o is None else t + o for o in offsets]
        if dot is not None:
            @pl.when(dot + DEEP < chunks)
            def _():
                load(lax.rem(dot + ahead + DEEP, chunks))
        if loads:
            @pl.when(jnp.logical_and(t >= DOWN_AT, t < chunks + DOWN_AT))
            def _():
                k = lax.rem(t - DOWN_AT + ahead, chunks)
                pltpu.make_async_copy(down_w.at[columns(k), :], down_v.at[k], d_sem.at[k]).start()
        if red is not None:
            core_copy(red).wait_recv()
            reduce_core(red)
            chip_copy(red).start()
        if act is not None:
            chip_copy(act).wait_recv()
            activate(act)
            hid_copy(act, my_rows).start()
            fwd_copy(act, my_rows).start()
        if fwd is not None:
            hid_copy(fwd, chip_rows).wait_recv()
            fwd_copy(fwd, chip_rows).start()
        if dwn is not None:
            k = place(dwn)[1]

            @pl.when(dwn < chunks)
            def _():
                pltpu.make_async_copy(down_w.at[pl.ds(0, width), :], down_v.at[k], d_sem.at[k]).wait()

            fwd_copy(dwn, their_half).wait_recv()
        if dot is not None:
            ready(dot)
            project(dot)
        if dwn is not None:
            down(dwn)
        if dot is not None:
            core_copy(dot).start()
        if dwn is not None:
            for c in range(1, n):
                @pl.when(dwn == leave[c])
                def _():
                    grid_out[c] = acc[c].astype(jnp.bfloat16)
                    grid_copy(c).start()
        return carry

    started()
    plan = {}
    for i in range(units):
        for stage, lag in enumerate(LAGS):
            plan.setdefault(i + lag, [None] * 5)[stage] = -lag
    steps = [tuple(plan.get(t, [None] * 5)) for t in range(max(plan) + 1)]
    low = 0
    for t in range(1, len(steps) + 1):
        if t == len(steps) or steps[t] != steps[low]:
            loads = low < chunks + DOWN_AT and t > DOWN_AT
            lax.fori_loop(low, t, functools.partial(step, steps[low], loads), 0)
            low = t

    total = acc[0]
    for s in range(1, n):
        grid_copy(s).wait_recv()
        total = total + grid_in[s].astype(jnp.float32)
    out[...] = total.astype(out.dtype)

    for s in range(1, n):
        tok_copy(s).wait_send()
        grid_copy(s).wait_send()

    def drain(ref, sem, device):
        pltpu.make_async_remote_copy(
            ref, ref, sem, corer_sem.at[0], device_id=device, device_id_type=MESH).wait_send()

    drain(core_out, cores_sem, other_core)
    drain(chip_out, chips_sem, other_chip)
    drain(hid.at[:, my_rows], hids_sem, other_chip)
    drain(hid.at[:, their_half], fwds_sem, other_core)


def fused(n, width, tokens, gate_weight, up_weight, down_weight):
    rows, feats = tokens.shape
    share, outs = down_weight.shape
    chunks = share // width
    units = n * chunks
    vmem, dma = pltpu.VMEM, pltpu.SemaphoreType.DMA
    bf, f4 = jnp.bfloat16, jnp.float32
    return pl.pallas_call(
        functools.partial(kernel, n, chunks, width),
        out_shape=pltpu.VMEM((rows, outs), bf),
        in_specs=[pl.BlockSpec(memory_space=pl.ANY)] * 4,
        out_specs=pl.BlockSpec(memory_space=pltpu.VMEM),
        scratch_shapes=[
            vmem((n, rows, feats), bf),
            vmem((chunks, feats, width), bf),
            vmem((chunks, feats, width), bf),
            vmem((chunks, width, outs), bf),
            vmem((units, rows // 2, 2 * width), f4),
            vmem((units, rows // 2, 2 * width), f4),
            vmem((units, rows // 2, 2 * width), f4),
            vmem((units, rows // 4, 2 * width), bf),
            vmem((units, rows // 4, 2 * width), bf),
            vmem((units, rows, width), bf),
            vmem((n, rows, outs), f4),
            vmem((n, rows, outs), bf),
            vmem((n, rows, outs), bf),
            dma((2 * chunks,)), dma((chunks,)), dma, dma((n,)), dma((n,)),
            dma, dma((RING,)), dma, dma((RING,)),
            dma, dma((RING,)), dma, dma((RING,)), dma((n,)), dma((n,)),
        ],
        compiler_params=pltpu.CompilerParams(
            collective_id=0, has_side_effects=True, vmem_limit_bytes=60 * 1024 * 1024),
    )(tokens, gate_weight, up_weight, down_weight)


def plain(tokens, gate_weight, up_weight, down_weight):
    grid_size = lax.axis_size("grid")
    block_rows = tokens.shape[0]
    total_rows = block_rows * grid_size
    width_share = gate_weight.shape[1]
    stacked = jnp.concatenate([gate_weight, up_weight], axis=1)
    pre_act = jnp.dot(
        lax.all_gather(tokens, "grid", axis=0, tiled=True), stacked, preferred_element_type=jnp.float32)
    blocked = pre_act.reshape(grid_size, block_rows, 2 * width_share)
    summed = lax.psum_scatter(blocked, "depth", scatter_dimension=1, tiled=True)
    hidden = lax.all_gather(
        (jax.nn.silu(summed[..., :width_share]) * summed[..., width_share:]).astype(jnp.bfloat16),
        "depth", axis=1, tiled=True,
    ).reshape(total_rows, width_share)
    return lax.psum_scatter(
        jnp.dot(hidden, down_weight, preferred_element_type=jnp.float32),
        "grid", scatter_dimension=0, tiled=True,
    ).astype(jnp.bfloat16)


def body(tokens, gate_weight, up_weight, down_weight):
    n, depth = lax.axis_size("grid"), lax.axis_size("depth")
    rows, share = tokens.shape[0], gate_weight.shape[1]
    width = next((w for w in (512, 256) if share % w == 0), None)
    weights = 2 * (2 * gate_weight.size + down_weight.size)
    if depth == 4 and n in (2, 4, 8) and rows == 64 and width and weights < 32 * 2**20:
        return fused(n, width, tokens, gate_weight, up_weight, down_weight)
    return plain(tokens, gate_weight, up_weight, down_weight)


def solution(mesh):
    placed = (
        P(("groups", "grid"), "depth"),
        P("depth", "grid"),
        P("depth", "grid"),
        P("grid", "depth"),
    )
    return jax.shard_map(
        body, mesh=mesh, in_specs=placed, out_specs=P(("groups", "grid"), "depth"), check_vma=False
    )
```
